8 devices in a mesh: emb: 8 (over z, y, x, core).
Axes of the slice: x: 2, y: 2, z: 1, core: 2. Of those that a mesh axis runs over, the one named last changes fastest.
Arguments:
- tok_ids: int32 [8192], P('emb')
- x_in: bfloat16 [8192, 768], P('emb')
- d_out: bfloat16 [8192, 768], P('emb')
- ple_tables: bfloat16 [5, 50304, 768], P(None, 'emb')
- w_up: bfloat16 [5, 768, 3072], replicated
- w_down: bfloat16 [5, 3072, 768], replicated
- w_gate: bfloat16 [5, 768, 768], replicated
- w_proj: bfloat16 [5, 768, 768], replicated
Outputs:
- output 1: bfloat16 [8192, 768], P('emb')
- output 2: float32 [5, 50304, 768], P(None, 'emb')
- output 3: float32 [5, 768, 3072], replicated
- output 4: float32 [5, 3072, 768], replicated
- output 5: float32 [5, 768, 768], replicated
- output 6: float32 [5, 768, 768], replicated
All inputs are finite; a program needn't handle non-finite values.
Results may differ from the reference program's by a relative error of at most 0.0177945.
Values are sent between devices in bfloat16 or wider.
A program may use at most 1.25 GiB of HBM per device.

```python
import math
import jax
import jax.numpy as jnp
from jax import lax

VOCAB_SIZE = 50304
MODEL_DIM = 768
HIDDEN_DIM = 3072
EMBED_DIM = 768
LAYERS = 5
TOKENS = 8192
SHARDS = 8

ROWS_DEV = VOCAB_SIZE // SHARDS
TOKENS_PER = TOKENS // SHARDS
CAP_ROWS = TOKENS_PER // 4
ROW_BITS = int(math.log2(ROWS_DEV)) + 1
EPS = 1e-6


def draw_ids(key):
    k_hot, k_off, k_row, k_shift, k_perm = jax.random.split(key, 5)
    hot_owner = jax.random.randint(k_hot, (SHARDS, 1), 0, SHARDS)
    start_off = jax.random.randint(k_off, (SHARDS, 1), 0, SHARDS - 1)
    slot_idx = jnp.arange(TOKENS_PER)[None, :]
    spread_owner = (hot_owner + 1 + (start_off + slot_idx - CAP_ROWS) % (SHARDS - 1)) % SHARDS
    owner_dev = jnp.where(slot_idx < CAP_ROWS, hot_owner, spread_owner)
    raw_rows = jax.random.randint(k_row, (SHARDS, TOKENS_PER), 0, ROWS_DEV)
    shift_bits = jax.random.randint(k_shift, (SHARDS, TOKENS_PER), 0, ROW_BITS + 1)
    local_row = jnp.right_shift(raw_rows, shift_bits)
    id_grid = owner_dev * ROWS_DEV + local_row
    id_grid = jax.random.permutation(k_perm, id_grid, axis=1, independent=True)
    return id_grid.reshape(TOKENS).astype(jnp.int32)


def draw_normal(key, shape, scale):
    return (jax.random.normal(key, shape, jnp.float32) * scale).astype(jnp.bfloat16)


def setup_inputs(seed: int = 0) -> dict:
    key_list = jax.random.split(jax.random.key(seed), 8)
    return {
        "tok_ids": draw_ids(key_list[0]),
        "x_in": draw_normal(key_list[1], (TOKENS, MODEL_DIM), 1.0),
        "d_out": draw_normal(key_list[2], (TOKENS, MODEL_DIM), 1.0),
        "ple_tables": draw_normal(key_list[3], (LAYERS, VOCAB_SIZE, EMBED_DIM), 1.0),
        "w_up": draw_normal(key_list[4], (LAYERS, MODEL_DIM, HIDDEN_DIM), MODEL_DIM ** -0.5),
        "w_down": draw_normal(key_list[5], (LAYERS, HIDDEN_DIM, MODEL_DIM), 0.5 * HIDDEN_DIM ** -0.5),
        "w_gate": draw_normal(key_list[6], (LAYERS, MODEL_DIM, EMBED_DIM), MODEL_DIM ** -0.5),
        "w_proj": draw_normal(key_list[7], (LAYERS, EMBED_DIM, MODEL_DIM), 0.35 * EMBED_DIM ** -0.5),
    }


def gelu_tanh(pre_act):
    return jax.nn.gelu(pre_act, approximate=True)


def gelu_back(pre_act, grad_out):
    _, pull_back = jax.vjp(gelu_tanh, pre_act.astype(jnp.float32))
    return pull_back(grad_out.astype(jnp.float32))[0]


def layer_fwd(x_cur, up_mat, down_mat, gate_mat, proj_mat, emb_rows):
    x_wide = x_cur.astype(jnp.float32)
    inv_rms = lax.rsqrt(jnp.mean(x_wide * x_wide, axis=-1, keepdims=True) + EPS)
    normed = (x_wide * inv_rms).astype(jnp.bfloat16)
    hidden = jnp.dot(normed, up_mat, preferred_element_type=jnp.float32).astype(jnp.bfloat16)
    act_out = gelu_tanh(hidden.astype(jnp.float32)).astype(jnp.bfloat16)
    mlp_out = jnp.dot(act_out, down_mat, preferred_element_type=jnp.float32).astype(jnp.bfloat16)
    gate_pre = jnp.dot(normed, gate_mat, preferred_element_type=jnp.float32).astype(jnp.bfloat16)
    gate_act = gelu_tanh(gate_pre.astype(jnp.float32)).astype(jnp.bfloat16)
    mix_rows = (gate_act.astype(jnp.float32) * emb_rows.astype(jnp.float32)).astype(jnp.bfloat16)
    ple_out = jnp.dot(mix_rows, proj_mat, preferred_element_type=jnp.float32).astype(jnp.bfloat16)
    x_next = (x_wide + mlp_out.astype(jnp.float32) + ple_out.astype(jnp.float32)).astype(jnp.bfloat16)
    return x_next, (x_wide, inv_rms, normed, hidden, act_out, gate_pre, gate_act, mix_rows)


def layer_bwd(d_x, saved, emb_rows, up_mat, down_mat, gate_mat, proj_mat):
    x_wide, inv_rms, normed, hidden, act_out, gate_pre, gate_act, mix_rows = saved
    g_out = d_x.astype(jnp.bfloat16)
    d_act = jnp.dot(g_out, down_mat.T, preferred_element_type=jnp.float32).astype(jnp.bfloat16)
    d_hidden = gelu_back(hidden, d_act).astype(jnp.bfloat16)
    d_mix = jnp.dot(g_out, proj_mat.T, preferred_element_type=jnp.float32).astype(jnp.bfloat16)
    d_rows = gate_act.astype(jnp.float32) * d_mix.astype(jnp.float32)
    d_gate_act = (emb_rows.astype(jnp.float32) * d_mix.astype(jnp.float32)).astype(jnp.bfloat16)
    d_gate_pre = gelu_back(gate_pre, d_gate_act).astype(jnp.bfloat16)
    d_norm = jnp.dot(d_hidden, up_mat.T, preferred_element_type=jnp.float32) + jnp.dot(d_gate_pre, gate_mat.T, preferred_element_type=jnp.float32)
    d_x_new = d_x + inv_rms * d_norm - inv_rms ** 3 * x_wide * jnp.mean(d_norm * x_wide, axis=-1, keepdims=True)
    g_up = jnp.dot(normed.T, d_hidden, preferred_element_type=jnp.float32)
    g_down = jnp.dot(act_out.T, g_out, preferred_element_type=jnp.float32)
    g_gate = jnp.dot(normed.T, d_gate_pre, preferred_element_type=jnp.float32)
    g_proj = jnp.dot(mix_rows.T, g_out, preferred_element_type=jnp.float32)
    return d_x_new, (g_up, g_down, g_gate, g_proj), d_rows


def reference(tok_ids, x_in, d_out, ple_tables, w_up, w_down, w_gate, w_proj):
    weights = (w_up, w_down, w_gate, w_proj)
    ids_blocks = tok_ids.reshape(SHARDS, TOKENS_PER)
    x_blocks = x_in.reshape(SHARDS, TOKENS_PER, MODEL_DIM)
    dy_blocks = d_out.reshape(SHARDS, TOKENS_PER, MODEL_DIM)

    def fwd_step(x_cur, layer_in):
        up_mat, down_mat, gate_mat, proj_mat, emb_rows = layer_in
        return layer_fwd(x_cur, up_mat, down_mat, gate_mat, proj_mat, emb_rows)

    def bwd_step(d_x, layer_in):
        saved, up_mat, down_mat, gate_mat, proj_mat, emb_rows = layer_in
        d_x_new, grads, d_rows = layer_bwd(d_x, saved, emb_rows, up_mat, down_mat, gate_mat, proj_mat)
        return d_x_new, (grads, d_rows)

    def block_step(carry, block_in):
        grad_acc, table_acc = carry
        blk_ids, blk_x, blk_dy = block_in
        rows_all = ple_tables[:, blk_ids, :]
        x_last, saved_all = lax.scan(fwd_step, blk_x, weights + (rows_all,))
        _, (grads, d_rows) = lax.scan(bwd_step, blk_dy.astype(jnp.float32), (saved_all,) + weights + (rows_all,), reverse=True)
        grad_acc = tuple(acc_part + new_part for acc_part, new_part in zip(grad_acc, grads))
        table_acc = table_acc.at[:, blk_ids, :].add(d_rows)
        return (grad_acc, table_acc), x_last

    grad_init = tuple(jnp.zeros(weight_mat.shape, jnp.float32) for weight_mat in weights)
    table_init = jnp.zeros(ple_tables.shape, jnp.float32)
    (grad_acc, table_acc), x_done = lax.scan(block_step, (grad_init, table_init), (ids_blocks, x_blocks, dy_blocks))
    x_out = x_done.reshape(TOKENS, MODEL_DIM)
    return (x_out, table_acc, grad_acc[0], grad_acc[1], grad_acc[2], grad_acc[3])
```

```python
import functools

import jax
import jax.numpy as jnp
from jax import lax
from jax.experimental import pallas as pl
from jax.experimental.pallas import tpu as pltpu
from jax.sharding import PartitionSpec as P

EPS = 1e-6
CAP_DIV = 4
CORES = 2
F32 = jnp.float32
BF16 = jnp.bfloat16
GELU_A = 0.7978845608028654
GELU_B = 0.044715 * GELU_A
VMEM_MAX = 67043328
TILE = 512
SPLIT = 3


def nn(a, b):
    return jnp.dot(a, b, preferred_element_type=F32)


def nt(a, b):
    return lax.dot_general(a, b, (((1,), (1,)), ((), ())), preferred_element_type=F32)


def tn(a, b):
    return lax.dot_general(a, b, (((0,), (0,)), ((), ())), preferred_element_type=F32)


def gelu_parts(h):
    sq = h * h
    return 0.5 * jnp.tanh(h * (GELU_B * sq + GELU_A)) + 0.5, sq


def gelu(h):
    return h * gelu_parts(h)[0]


def gelu_slope(h, half, sq):
    return half + (h * (half - half * half)) * ((6 * GELU_B) * sq + 2 * GELU_A)


def norm_rows(x_ref):
    xw = x_ref[...].astype(F32)
    r = lax.rsqrt(jnp.mean(xw * xw, axis=-1, keepdims=True) + EPS)
    return xw, r, (xw * r).astype(BF16)


def token_spec(tile, width):
    return pl.BlockSpec((tile, width), lambda i: (i, 0))


def weight_spec(arr, layer):
    return pl.BlockSpec((None,) + arr.shape[1:], lambda i: (layer, 0, 0), pipeline_mode=pl.Buffered(1))


def fwd_kernel(chunk, x_ref, e_ref, up_ref, down_ref, gate_ref, proj_ref, out_ref):
    xw, _, u = norm_rows(x_ref)
    z = nn(u, gate_ref[...]).astype(BF16).astype(F32)
    s = (gelu(z).astype(BF16).astype(F32) * e_ref[...].astype(F32)).astype(BF16)
    m = None
    for k in range(up_ref.shape[1] // chunk):
        cols = pl.ds(k * chunk, chunk)
        a = gelu(nn(u, up_ref[:, cols]).astype(BF16).astype(F32)).astype(BF16)
        part = nn(a, down_ref[cols, :])
        m = part if m is None else m + part
    q = nn(s, proj_ref[...]).astype(BF16)
    out_ref[...] = (xw + m.astype(BF16).astype(F32) + q.astype(F32)).astype(BF16)


def layer_fwd(layer, x, e, weights, tile=TILE, chunk=1024):
    n, d = x.shape
    f = weights[0].shape[2]
    return pl.pallas_call(
        functools.partial(fwd_kernel, chunk),
        grid=(n // tile,),
        in_specs=[token_spec(tile, d)] * 2 + [weight_spec(w, layer) for w in weights],
        out_specs=token_spec(tile, d),
        out_shape=jax.ShapeDtypeStruct((n, d), BF16),
        compiler_params=pltpu.CompilerParams(vmem_limit_bytes=48 << 20),
        cost_estimate=pl.CostEstimate(flops=4 * n * d * (f + d), bytes_accessed=4 * d * (f + d), transcendentals=n * (f + d)),
        name="layer_fwd",
    )(x, e, *weights)


def gather_kernel(unroll, cnt_ref, idx_ref, table_ref, out_ref, rows, tmp):
    homes, cap = idx_ref.shape
    for h in range(homes):

        def body(t, _, h=h):
            for v in range(unroll):
                j = t * unroll + v
                r = idx_ref[h, j]
                tmp[v] = table_ref[pl.ds(pl.multiple_of(r - (r & 7), 8), 8), :].astype(F32)
                rows[pl.ds(h * cap + j, 1), :] = tmp[v, pl.ds(r & 7, 1), :]
            return 0

        lax.fori_loop(0, (cnt_ref[h] + unroll - 1) // unroll, body, 0)
    out_ref[...] = rows[...].astype(BF16)


def serve_rows(tables, first, count, cnt, idx, unroll=16):
    _, rows, d = tables.shape
    homes, cap = idx.shape
    return pl.pallas_call(
        functools.partial(gather_kernel, unroll),
        grid_spec=pltpu.PrefetchScalarGridSpec(
            num_scalar_prefetch=2,
            grid=(count,),
            in_specs=[pl.BlockSpec((None, rows, d), lambda i, *_: (first + i, 0, 0))],
            out_specs=pl.BlockSpec((None, homes * cap, d), lambda i, *_: (i, 0, 0)),
            scratch_shapes=[pltpu.VMEM((homes * cap, d), F32), pltpu.VMEM((unroll, 8, d), F32)],
        ),
        out_shape=jax.ShapeDtypeStruct((count, homes * cap, d), BF16),
        compiler_params=pltpu.CompilerParams(vmem_limit_bytes=48 << 20),
        cost_estimate=pl.CostEstimate(flops=count * 10**9, bytes_accessed=2 * count * rows * d, transcendentals=0),
        name="serve_rows",
    )(cnt, idx, tables)


def bwd_kernel(chunk, last, seeded, extra, chip_ref, *refs):
    x_ref, e_ref, c_ref, up_ref, down_ref, gate_ref, proj_ref = refs[:7]
    outs = refs[7 + extra:]
    seeds = refs[7:7 + seeded]
    if last:
        gds_ref, gup_ref, gdown_ref, ggate_ref, gproj_ref = outs[:5]
    else:
        cn_ref, gds_ref, gup_ref, gdown_ref, ggate_ref, gproj_ref = outs[:6]
    sem = outs[-1]

    @pl.when(pl.program_id(0) == 0)
    def _():
        accs = (gup_ref, gdown_ref, ggate_ref, gproj_ref)
        if seeded:
            copies = [pltpu.make_async_copy(seeds[k], accs[k], sem.at[k]) for k in range(4)]
            for copy in copies:
                copy.start()
            for copy in copies:
                copy.wait()
        else:
            for ref in accs:
                ref[...] = jnp.zeros_like(ref)

    xw, r, u = norm_rows(x_ref)
    c = c_ref[...].astype(F32)
    o = c.astype(BF16)
    steps = up_ref.shape[1] // chunk

    def first(k):
        cols = pl.ds(k * chunk, chunk)
        return nt(o, down_ref[cols, :]).astype(BF16), nn(u, up_ref[:, cols]).astype(BF16)

    def middle(da, h):
        h = h.astype(F32)
        half, sq = gelu_parts(h)
        return (gelu_slope(h, half, sq) * da.astype(F32)).astype(BF16), (h * half).astype(BF16)

    def final(k, dh, a):
        cols = pl.ds(k * chunk, chunk)
        gup_ref[:, cols] += tn(u, dh)
        gdown_ref[cols, :] += tn(a, o)
        return None if last else nt(dh, up_ref[:, cols])

    pre = first(0)
    z = nn(u, gate_ref[...]).astype(BF16).astype(F32)
    ds = nt(o, proj_ref[...]).astype(BF16).astype(F32)
    e = e_ref[...].astype(F32)
    half, sq = gelu_parts(z)
    g = (z * half).astype(BF16).astype(F32)
    gds_ref[...] = g * ds
    s = (g * e).astype(BF16)
    dz = (gelu_slope(z, half, sq) * (e * ds).astype(BF16).astype(F32)).astype(BF16)
    ggate_ref[...] += tn(u, dz)
    gproj_ref[...] += tn(s, o)
    du = None if last else nt(dz, gate_ref[...])
    mid = None
    for k in range(steps):
        nxt = first(k + 1) if k + 1 < steps else None
        if mid is not None:
            part = final(k - 1, *mid)
            du = None if last else du + part
        mid = middle(*pre)
        pre = nxt
    part = final(steps - 1, *mid)
    if not last:
        du = du + part
        cn_ref[...] = c + r * du - (r * r * r) * xw * jnp.mean(du * xw, axis=-1, keepdims=True)


def layer_bwd(layer, chip, span, total, x, e, c, weights, seed=None, gds=None, c_out=None, c_total=None, tile=TILE, chunk=768):
    d = x[0].shape[1]
    f = weights[0].shape[2]
    last = layer == 0
    struct = jax.ShapeDtypeStruct
    lo, hi = span[0] // tile, span[1] // tile
    block = total // 4 // tile

    def place(kind):
        if kind == "local":
            return pl.BlockSpec((tile, d), lambda i, chip: (i, 0))
        if kind == "ordered":
            return pl.BlockSpec((tile, d), lambda i, chip: (i + lo, 0))

        def index(i, chip):
            t = i + lo
            b = t // block
            b = jnp.where(b == 0, chip[0], jnp.where(b <= chip[0], b - 1, b))
            return (b * block + t % block, 0)

        return pl.BlockSpec((tile, d), index)

    any_spec = pl.BlockSpec(memory_space=pl.ANY)
    wspec = lambda w: pl.BlockSpec((None,) + w.shape[1:], lambda i, chip: (layer, 0, 0), pipeline_mode=pl.Buffered(1))
    whole = lambda shape: pl.BlockSpec(shape, lambda i, chip: (0, 0), pipeline_mode=pl.Buffered(1))
    grads = [(d, f), (f, d), (d, d), (d, d)]
    args = [chip, x[0], e[0], c[0], *weights]
    in_specs = [place(x[1]), place(e[1]), place(c[1])] + [wspec(w) for w in weights]
    aliases = {}
    if seed is not None:
        args += list(seed)
        in_specs += [any_spec] * 4
    n_c = 0 if last else 1
    for buf, pos in ((c_out, 0), (gds, n_c)):
        if buf is not None:
            aliases[len(args)] = pos
            args.append(buf)
            in_specs.append(any_spec)
    rows_out, rows_spec = [], []
    if not last:
        rows_out.append(struct((c_total or (span[1] - span[0]), d), F32))
        rows_spec.append(place("ordered" if c_total else "local"))
    rows_out.append(struct((total, d), F32))
    rows_spec.append(place("ordered"))
    extra = len(args) - 8
    n = span[1] - span[0]
    res = pl.pallas_call(
        functools.partial(bwd_kernel, chunk, last, 0 if seed is None else 4, extra),
        grid_spec=pltpu.PrefetchScalarGridSpec(
            num_scalar_prefetch=1,
            grid=(hi - lo,),
            in_specs=in_specs,
            out_specs=rows_spec + [whole(g) for g in grads],
            scratch_shapes=[pltpu.SemaphoreType.DMA((4,))],
        ),
        out_shape=rows_out + [struct(g, F32) for g in grads],
        input_output_aliases=aliases,
        compiler_params=pltpu.CompilerParams(vmem_limit_bytes=VMEM_MAX),
        cost_estimate=pl.CostEstimate(flops=10 * n * d * (f + d), bytes_accessed=12 * d * (f + d), transcendentals=n * (f + d)),
        name="layer_bwd",
    )(*args)
    return (None if last else res[0]), res[-5], tuple(res[-4:])


def table_kernel(first, layers, seg, unroll, cnt_ref, start_ref, dst_ref, *refs):
    mine, other = refs[:layers], refs[layers:2 * layers]
    out_ref, acc, buf, in_sem, out_sem = refs[-5:]
    homes = dst_ref.shape[0]
    half = homes // 2
    total = mine[0].shape[0]
    toks = total // half

    def base(h):
        return jnp.minimum(start_ref[h] - start_ref[h] % 8, toks - seg)

    def load(l, h):
        ref = mine[l] if h < half else other[l]
        at = pl.multiple_of((h % half) * toks + base(h), 8)
        return pltpu.make_async_copy(ref.at[pl.ds(at, seg), :], buf.at[l % 2, h], in_sem.at[l % 2, h])

    def store(l):
        return pltpu.make_async_copy(acc.at[l % 2], out_ref.at[first - l], out_sem.at[l % 2])

    for h in range(homes):
        load(0, h).start()
    for l in range(layers):
        if l + 1 < layers:
            for h in range(homes):
                load(l + 1, h).start()
        if l >= 2:
            store(l - 2).wait()
        acc[l % 2] = jnp.zeros_like(acc[l % 2])
        for h in range(homes):
            load(l, h).wait()
            off = start_ref[h] - base(h)

            def add(j, h=h, l=l, off=off):
                at = pl.ds(dst_ref[h, j], 1)
                acc[l % 2, at, :] += buf[l % 2, h, pl.ds(off + j, 1), :]

            def many(t, _, add=add):
                for v in range(unroll):
                    add(t * unroll + v)
                return 0

            def one(j, _, add=add):
                add(j)
                return 0

            full = cnt_ref[h] // unroll
            lax.fori_loop(0, full, many, 0)
            lax.fori_loop(full * unroll, cnt_ref[h], one, 0)
        store(l).start()
    for l in range(max(layers - 2, 0), layers):
        store(l).wait()


def table_grad(first, layers_all, rows, cnt, start, dst, mine, other, prev):
    d = mine[0].shape[1]
    homes, cap = dst.shape
    seg = cap + 8
    any_spec = pl.BlockSpec(memory_space=pl.ANY)
    args = [cnt, start, dst, *mine, *other]
    aliases = {}
    if prev is not None:
        aliases = {len(args): 0}
        args.append(prev)
    return pl.pallas_call(
        functools.partial(table_kernel, first, len(mine), seg, 8),
        grid_spec=pltpu.PrefetchScalarGridSpec(
            num_scalar_prefetch=3,
            in_specs=[any_spec] * (len(args) - 3),
            out_specs=any_spec,
            scratch_shapes=[
                pltpu.VMEM((2, rows, d), F32),
                pltpu.VMEM((2, homes, seg, d), F32),
                pltpu.SemaphoreType.DMA((2, homes)),
                pltpu.SemaphoreType.DMA((2,)),
            ],
        ),
        out_shape=jax.ShapeDtypeStruct((layers_all, rows, d), F32),
        input_output_aliases=aliases,
        compiler_params=pltpu.CompilerParams(vmem_limit_bytes=VMEM_MAX),
        cost_estimate=pl.CostEstimate(flops=len(mine) * 10**9, bytes_accessed=8 * len(mine) * rows * d, transcendentals=0),
        name="table_grad",
    )(*args)


def sum_kernel(count, *refs):
    outs = refs[-count:]
    for k in range(count):
        outs[k][...] = refs[k][...] + refs[count + k][...]


def sum_grads(layer, layers, mine, other, prev, steps=8):
    count = len(mine)
    ins, outs = [], []
    for arr in mine:
        block = (arr.shape[0] // steps, arr.shape[1])
        ins.append(pl.BlockSpec(block, lambda i: (i, 0)))
        outs.append(pl.BlockSpec((None,) + block, lambda i: (layer, i, 0)))
    args = list(mine) + list(other)
    aliases = {}
    if prev is not None:
        aliases = {len(args) + k: k for k in range(count)}
        args += list(prev)
    return pl.pallas_call(
        functools.partial(sum_kernel, count),
        grid=(steps,),
        in_specs=ins + ins + [pl.BlockSpec(memory_space=pl.ANY)] * len(aliases),
        out_specs=outs,
        out_shape=[jax.ShapeDtypeStruct((layers,) + arr.shape, F32) for arr in mine],
        input_output_aliases=aliases,
        compiler_params=pltpu.CompilerParams(vmem_limit_bytes=32 << 20),
        cost_estimate=pl.CostEstimate(flops=10**9, bytes_accessed=12 * sum(a.size for a in mine), transcendentals=0),
        name="sum_grads",
    )(*args)


def after(value, *deps):
    return lax.optimization_barrier((value,) + deps)[0]


def solution(mesh):
    shards = mesh.shape["emb"]
    chips = shards // CORES
    same_core = [[chip * CORES + core for chip in range(chips)] for core in range(CORES)]
    swap = [(d, d ^ 1) for d in range(shards)]

    def device_step(tok_ids, x_in, d_out, ple_tables, w_up, w_down, w_gate, w_proj):
        layers, rows_dev, width = ple_tables.shape
        toks = tok_ids.shape[0]
        total = toks * chips
        cap = toks // CAP_DIV
        me = lax.axis_index("emb")
        core, chip = me % CORES, me // CORES
        weights = (w_up, w_down, w_gate, w_proj)
        i32 = jnp.int32

        def gather_core(arr):
            return lax.all_gather(arr, "emb", axis_index_groups=same_core, tiled=True)

        owner = tok_ids // rows_dev
        local_row = tok_ids - owner * rows_dev
        hot = (owner[:, None] == jnp.arange(shards, dtype=i32)[None, :]).astype(i32)
        run = jnp.cumsum(hot, axis=0)
        rank = jnp.sum((run - hot) * hot, axis=1)
        counts = run[-1]
        starts = jnp.cumsum(counts) - counts
        pos = jnp.sum(starts[None, :] * hot, axis=1) + rank
        perm = jnp.zeros((toks,), i32).at[pos].set(jnp.arange(toks, dtype=i32))
        req = jnp.zeros((shards * 2 * cap,), i32).at[owner * (2 * cap) + rank].set(local_row).reshape(shards, 2 * cap)
        req = req.at[:, cap].set(counts).at[:, cap + 1].set(starts)
        req = lax.all_to_all(req, "emb", 0, 0, tiled=True)
        want, cnt, start = req[:, :cap], req[:, cap], req[:, cap + 1]

        x_own = [x_in.at[perm].get(mode="promise_in_bounds")]
        dy_own = d_out.at[perm].get(mode="promise_in_bounds")

        rel = jnp.arange(shards, dtype=i32) ^ me
        cnt_rel, want_rel = cnt[rel], want[rel]
        take = ((owner ^ me) * cap + rank)[perm]

        served = [serve_rows(ple_tables, 0, 1, cnt_rel, want_rel)[0]]
        for l in range(1, layers):
            served.append(serve_rows(ple_tables, l, 1, after(cnt_rel, served[l - 1]), want_rel)[0])
        own_rows = []
        for l in range(layers):
            rows = served[l].reshape(shards, cap, width)
            got = [rows[0]] + [lax.ppermute(rows[s], "emb", [(d, d ^ s) for d in range(shards)]) for s in range(1, shards)]
            if l > 0:
                got[0] = after(got[0], x_own[l])
            own_rows.append(jnp.concatenate(got).at[take].get(mode="promise_in_bounds"))
            x_own.append(layer_fwd(l, x_own[l], own_rows[l], weights))

        chip_arr = chip.astype(i32)[None]
        own, oth, every = (0, toks), (toks, total), (0, total)
        split = layers - SPLIT
        c_own = [None] * (layers + 1)
        c_own[layers] = dy_own
        seeds, gds_buf = {}, {}
        c_rel = None
        for l in reversed(range(split, layers)):
            edge = l == split
            res = layer_bwd(l, chip_arr, own, total, (x_own[l], "local"), (own_rows[l], "local"), (c_own[l + 1], "local"), weights, c_total=total if edge else None)
            c_own[l], gds_buf[l], seeds[l] = res
            if edge:
                c_rel = res[0]
        ready = own_rows[layers - 1]
        dy_all = gather_core(after(dy_own, ready))
        c, kind = after(dy_all, gds_buf[split]), "all"
        gds, part, other = {}, {}, {}
        swapped, sums = {}, None
        for l in reversed(range(layers)):
            e_all = gather_core(after(own_rows[l], ready))
            x_all = gather_core(after(x_own[l], ready))
            xe = ((x_all, "all"), (e_all, "all"))
            if l >= split:
                edge = l == split
                c_new, gds[l], part[l] = layer_bwd(l, chip_arr, oth, total, *xe, (c, kind), weights, seed=seeds[l], gds=gds_buf[l], c_out=c_rel if edge else None, c_total=total if edge else None)
            else:
                c_new, gds[l], part[l] = layer_bwd(l, chip_arr, every, total, *xe, (c, "local"), weights, c_total=total)
            kind = "local"
            swapped[l] = tuple(lax.ppermute(p, "emb", swap) for p in part[l])
            other[l] = lax.ppermute(gds[l], "emb", swap)
            if l + 1 < layers:
                held = lax.optimization_barrier((gds[l], other[l + 1], swapped[l + 1]))
                other[l + 1] = held[1]
                sums = sum_grads(l + 1, layers, part[l + 1], held[2], sums)
                if l > 0:
                    c_new, other[l + 1], sums = lax.optimization_barrier((c_new, other[l + 1], sums))
            c = c_new

        order = jnp.arange(chips, dtype=i32)
        order = jnp.where(order == 0, chip, jnp.where(order <= chip, order - 1, order)) * CORES
        order = jnp.concatenate([order + core, order + 1 - core])
        lists = (cnt[order], start[order], want[order])
        upper = list(range(layers - 1, 0, -1))
        tables = table_grad(layers - 1, layers, rows_dev, *lists, [after(gds[l], gds[0]) for l in upper], [other[l] for l in upper], None)
        sums = sum_grads(0, layers, part[0], after(swapped[0], tables), sums)
        tables = table_grad(0, layers, rows_dev, *lists, [gds[0]], [other[0]], tables)
        x_out = x_own[layers].at[pos].get(mode="promise_in_bounds")
        return (x_out, tables, *sums)

    return jax.shard_map(
        device_step,
        mesh=mesh,
        in_specs=(P("emb"), P("emb", None), P("emb", None), P(None, "emb", None), P(), P(), P(), P()),
        out_specs=(P("emb", None), P(None, "emb", None), P(), P(), P(), P()),
        check_vma=False,
    )
```

```python
import functools

import jax
import jax.numpy as jnp
from jax import lax
from jax.experimental import pallas as pl
from jax.experimental.pallas import tpu as pltpu
from jax.sharding import PartitionSpec as P


EPS = 1e-6
CAP_DIV = 4
CORES = 2
F32 = jnp.float32
BF16 = jnp.bfloat16
GELU_A = 0.7978845608028654
GELU_B = 0.044715 * GELU_A
VMEM_MAX = 67043328
TILE = 512
MEMORY_UNIT = 500000000
SPLIT = 3
SPREAD = (3, 2, 1)


def nn(a, b):
    return jnp.dot(a, b, preferred_element_type=F32)


def nt(a, b):
    return lax.dot_general(a, b, (((1,), (1,)), ((), ())), preferred_element_type=F32)


def tn(a, b):
    return lax.dot_general(a, b, (((0,), (0,)), ((), ())), preferred_element_type=F32)


def gelu_parts(h):
    sq = h * h
    return 0.5 * jnp.tanh(h * (GELU_B * sq + GELU_A)) + 0.5, sq


def gelu(h):
    return h * gelu_parts(h)[0]


def gelu_slope(h, half, sq):
    return half + (h * (half - half * half)) * ((6 * GELU_B) * sq + 2 * GELU_A)


def norm_rows(x_ref):
    xw = x_ref[...].astype(F32)
    r = lax.rsqrt(jnp.mean(xw * xw, axis=-1, keepdims=True) + EPS)
    return xw, r, (xw * r).astype(BF16)


def memory_cost(units):
    return pl.CostEstimate(flops=units * MEMORY_UNIT, bytes_accessed=units * MEMORY_UNIT, transcendentals=0)


def forward_rows(chunk, x_ref, e, w_ref):
    up_ref, down_ref, gate_ref, proj_ref = w_ref
    xw, _, u = norm_rows(x_ref)
    z = nn(u, gate_ref[...]).astype(BF16).astype(F32)
    s = (gelu(z).astype(BF16).astype(F32) * e.astype(F32)).astype(BF16)
    m = None
    for k in range(up_ref.shape[1] // chunk):
        cols = pl.ds(k * chunk, chunk)
        a = gelu(nn(u, up_ref[:, cols]).astype(BF16).astype(F32)).astype(BF16)
        part = nn(a, down_ref[cols, :])
        m = part if m is None else m + part
    q = nn(s, proj_ref[...]).astype(BF16)
    return (xw + m.astype(BF16).astype(F32) + q.astype(F32)).astype(BF16)


def start_kernel(chunk, tile, shards, take_ref, x_ref, served_ref, *refs):
    got, refs = refs[:shards], refs[shards:]
    w_ref, refs = refs[:4], refs[4:]
    layer = pl.program_id(0)
    layers = served_ref.shape[0] + 1
    both_out = refs[:layers]
    recv, pick, x_cur, e_buf, x_buf, send_sem, recv_sem, own_sem, e_sem, x_sem, first_sem = refs[layers:]
    slots = served_ref.shape[1]
    toks = x_ref.shape[0]
    cap = slots // shards
    me = lax.axis_index("emb")

    def copy_in(l, s):
        rows = pl.ds(s * cap, cap)
        dst = recv.at[l, rows, :]
        if l == 0:
            return pltpu.make_async_copy(got[s], dst, first_sem.at[s])
        src = served_ref.at[l - 1, rows, :]
        if s == 0:
            return pltpu.make_async_copy(src, dst, own_sem.at[l])
        peer, bit = 0, 1
        while bit < shards:
            peer = peer + bit * ((me // bit + s // bit) % 2)
            bit *= 2
        return pltpu.make_async_remote_copy(
            src_ref=src,
            dst_ref=dst,
            send_sem=send_sem.at[l, s - 1],
            recv_sem=recv_sem.at[l, s - 1],
            device_id=(peer,),
            device_id_type=pl.DeviceIdType.MESH,
        )

    def save_e(l):
        return pltpu.make_async_copy(e_buf.at[l % 2], both_out[l].at[pl.ds(toks, toks), :], e_sem.at[l])

    def save_x(l):
        src = x_ref if l < 0 else x_buf.at[l % 2]
        return pltpu.make_async_copy(src, both_out[l + 1].at[pl.ds(0, toks), :], x_sem.at[l + 1])

    @pl.when(layer == 0)
    def _():
        for l in range(layers):
            for s in range(shards):
                copy_in(l, s).start()
        save_x(-1).start()
        x_cur[...] = x_ref[...]
        lanes = lax.broadcasted_iota(jnp.int32, (toks, cap), 1)
        for k in range(shards):
            pick[:, pl.ds(k * cap, cap)] = jnp.where(take_ref[...] == lanes + k * cap, 1.0, 0.0).astype(BF16)

    for l in range(layers):

        @pl.when(layer == l)
        def _(l=l):
            copy_in(l, 0).wait()
            for s in range(1, shards):
                copy_in(l, s).wait_recv() if l else copy_in(l, s).wait()
            if l >= 2:
                save_e(l - 2).wait()
                save_x(l - 2).wait()

    half = layer % 2
    e_buf[half] = nn(pick[...], recv[layer]).astype(BF16)

    @pl.when(layer < layers - 1)
    def _():
        for t in range(toks // tile):
            rows = pl.ds(t * tile, tile)
            x_new = forward_rows(chunk, x_cur.at[rows, :], e_buf[half, rows, :], w_ref)
            x_buf[half, rows, :] = x_new
            x_cur[rows, :] = x_new

    for l in range(layers):

        @pl.when(layer == l)
        def _(l=l):
            save_e(l).start()
            if l < layers - 1:
                save_x(l).start()

    @pl.when(layer == layers - 1)
    def _():
        for l in range(1, layers):
            for s in range(1, shards):
                copy_in(l, s).wait_send()
        save_x(-1).wait()
        save_e(layers - 2).wait()
        save_x(layers - 2).wait()
        save_e(layers - 1).wait()


def start_layers(take, x, served, got, weights, shards, tile=TILE, chunk=1024):
    n, d = x.shape
    layers, slots = served.shape[0] + 1, served.shape[1]
    any_spec = pl.BlockSpec(memory_space=pl.ANY)
    whole = lambda arr: pl.BlockSpec(arr.shape, lambda i: (0, 0), pipeline_mode=pl.Buffered(1))
    wspec = lambda w: pl.BlockSpec((None,) + w.shape[1:], lambda i: (i, 0, 0))
    return pl.pallas_call(
        functools.partial(start_kernel, chunk, tile, shards),
        grid=(layers,),
        in_specs=[whole(take), whole(x)] + [any_spec] * (1 + shards) + [wspec(w) for w in weights],
        out_specs=[any_spec] * layers,
        out_shape=[jax.ShapeDtypeStruct((2 * n, d), BF16)] * layers,
        scratch_shapes=[
            pltpu.VMEM((layers, slots, d), BF16),
            pltpu.VMEM((n, slots), BF16),
            pltpu.VMEM((n, d), BF16),
            pltpu.VMEM((2, n, d), BF16),
            pltpu.VMEM((2, n, d), BF16),
            pltpu.SemaphoreType.DMA((layers, shards - 1)),
            pltpu.SemaphoreType.DMA((layers, shards - 1)),
            pltpu.SemaphoreType.DMA((layers,)),
            pltpu.SemaphoreType.DMA((layers,)),
            pltpu.SemaphoreType.DMA((layers,)),
            pltpu.SemaphoreType.DMA((shards,)),
        ],
        compiler_params=pltpu.CompilerParams(vmem_limit_bytes=VMEM_MAX, has_side_effects=True),
        cost_estimate=memory_cost(100),
        name="start_layers",
    )(take, x, served, *got, *weights)


def top_kernel(chunk, tile, pos_ref, x_ref, e_ref, *refs):
    w_ref, (out_ref, last, pick) = refs[:4], refs[4:]
    n = pos_ref.shape[1]
    for t in range(n // tile):
        rows = pl.ds(t * tile, tile)
        last[rows, :] = forward_rows(chunk, x_ref.at[rows, :], e_ref[rows, :], w_ref)
    pick_rows(pos_ref, pick)
    out_ref[...] = tn(pick[...], last[...]).astype(BF16)


def top_forward(pos, both, weights, tile=TILE, chunk=1024):
    n, d = both.shape[0] // 2, both.shape[1]
    half = lambda under: pl.BlockSpec((n, d), lambda i: (under, 0))
    wspec = lambda w: pl.BlockSpec((None,) + w.shape[1:], lambda i: (w.shape[0] - 1, 0, 0))
    row = pl.BlockSpec((1, n), lambda i: (0, 0))
    return pl.pallas_call(
        functools.partial(top_kernel, chunk, tile),
        grid=(1,),
        in_specs=[row, half(0), half(1)] + [wspec(w) for w in weights],
        out_specs=half(0),
        out_shape=jax.ShapeDtypeStruct((n, d), BF16),
        scratch_shapes=[pltpu.VMEM((n, d), BF16), pltpu.VMEM((n, n), BF16)],
        compiler_params=pltpu.CompilerParams(vmem_limit_bytes=VMEM_MAX),
        cost_estimate=memory_cost(30),
        name="top_forward",
    )(pos[None, :], both, both, *weights)


def gather_kernel(unroll, order_ref, idx_ref, table_ref, out_ref, rows, tmp):
    homes, cap = idx_ref.shape[0], idx_ref.shape[1] // 2

    @pl.when(pl.program_id(0) == 0)
    def _():
        rows[...] = jnp.zeros_like(rows)

    for h in range(homes):
        home = order_ref[h]

        def body(t, _, h=h, home=home):
            for v in range(unroll):
                j = t * unroll + v
                r = idx_ref[home, j]
                tmp[v] = table_ref[pl.ds(pl.multiple_of(r - (r & 7), 8), 8), :].astype(F32)
                rows[pl.ds(h * cap + j, 1), :] = tmp[v, pl.ds(r & 7, 1), :]
            return 0

        lax.fori_loop(0, (idx_ref[home, cap] + unroll - 1) // unroll, body, 0)
    out_ref[...] = rows[...].astype(BF16)


def serve_rows(tables, first, count, order, lists, unroll=16):
    _, rows, d = tables.shape
    homes, cap = lists.shape[0], lists.shape[1] // 2
    return pl.pallas_call(
        functools.partial(gather_kernel, unroll),
        grid_spec=pltpu.PrefetchScalarGridSpec(
            num_scalar_prefetch=2,
            grid=(count,),
            in_specs=[pl.BlockSpec((None, rows, d), lambda i, *_: (first + i, 0, 0))],
            out_specs=pl.BlockSpec((None, homes * cap, d), lambda i, *_: (i, 0, 0)),
            scratch_shapes=[pltpu.VMEM((homes * cap, d), F32), pltpu.VMEM((unroll, 8, d), F32)],
        ),
        out_shape=jax.ShapeDtypeStruct((count, homes * cap, d), BF16),
        compiler_params=pltpu.CompilerParams(vmem_limit_bytes=48 << 20),
        cost_estimate=memory_cost(2 * count),
        name="serve_rows",
    )(order, lists, tables)


def bwd_kernel(chunk, last, seeded, spread, extra, meta_ref, *refs):
    x_ref, e_ref, c_ref = refs[:3]
    w_hbm, seed_hbm = refs[3:7], refs[7:7 + 4 * seeded]
    refs = list(refs[7 + extra:])
    cn_ref = None if last else refs.pop(0)
    gds_ref, *refs = refs
    grad_hbm, w_ref, g_ref, (w_sem, s_sem, g_sem, *keep) = refs[:4], refs[4:8], refs[8:12], refs[12:]
    up_ref, down_ref, gate_ref, proj_ref = w_ref
    steps = up_ref.shape[1] // chunk
    step, n_steps = pl.program_id(0), pl.num_programs(0)
    cols = lambda k: pl.ds(k * chunk, chunk)

    def flush(a, k):
        part = lambda ref: ref if k is None else (ref.at[:, cols(k)] if a == 0 else ref.at[cols(k), :])
        return pltpu.make_async_copy(part(g_ref[a]), part(grad_hbm[a]), g_sem.at[a if k is None else 4 + 2 * k + a])

    @pl.when(step == 0)
    def _():
        loads = [pltpu.make_async_copy(w_hbm[a].at[meta_ref[1]], w_ref[a], w_sem.at[a]) for a in range(4)]
        loads += [pltpu.make_async_copy(seed_hbm[a], g_ref[a], s_sem.at[a]) for a in range(4 * seeded)]
        for load in loads:
            load.start()
        if not seeded:
            for ref in g_ref:
                ref[...] = jnp.zeros_like(ref)
        for load in loads:
            load.wait()

    started = []

    def accumulate(a, value, k=None):
        if k is None:
            g_ref[a][...] += value
        elif a == 0:
            g_ref[a][:, cols(k)] += value
        else:
            g_ref[a][cols(k), :] += value
        pl.when(step == n_steps - 1)(lambda: flush(a, k).start())
        started.append((a, k))

    xw, r, u = norm_rows(x_ref)
    c = c_ref[...].astype(F32)
    o = c.astype(BF16)

    def first(k):
        return nt(o, down_ref[cols(k), :]).astype(BF16), nn(u, up_ref[:, cols(k)]).astype(BF16)

    def middle(da, h):
        h = h.astype(F32)
        half, sq = gelu_parts(h)
        return (gelu_slope(h, half, sq) * da.astype(F32)).astype(BF16), (h * half).astype(BF16)

    def final(k, dh, a):
        if spread:
            keep[0][:, cols(k)] = dh
            keep[1][:, cols(k)] = a
        else:
            accumulate(0, tn(u, dh), k)
            accumulate(1, tn(a, o), k)
        return None if last else nt(dh, up_ref[:, cols(k)])

    pre = first(0)
    z = nn(u, gate_ref[...]).astype(BF16).astype(F32)
    ds = nt(o, proj_ref[...]).astype(BF16).astype(F32)
    e = e_ref[...].astype(F32)
    half, sq = gelu_parts(z)
    g = (z * half).astype(BF16).astype(F32)
    gds_ref[...] = g * ds
    s = (g * e).astype(BF16)
    dz = (gelu_slope(z, half, sq) * (e * ds).astype(BF16).astype(F32)).astype(BF16)
    accumulate(2, tn(u, dz))
    accumulate(3, tn(s, o))
    du = None if last else nt(dz, gate_ref[...])
    mid = None
    for k in range(steps):
        nxt = first(k + 1) if k + 1 < steps else None
        if mid is not None:
            part = final(k - 1, *mid)
            du = None if last else du + part
        mid = middle(*pre)
        pre = nxt
    part = final(steps - 1, *mid)
    if spread:
        width = g_ref[1].shape[0]
        mine = pl.ds(pl.multiple_of(meta_ref[0] * width, 128), width)
        accumulate(0, tn(u, keep[0][:, mine]))
        accumulate(1, tn(keep[1][:, mine], o))
    if not last:
        du = du + part
        cn_ref[...] = c + r * du - (r * r * r) * xw * jnp.mean(du * xw, axis=-1, keepdims=True)

    @pl.when(step == n_steps - 1)
    def _():
        for a, k in started:
            flush(a, k).wait()


def layer_bwd(layer, meta, which, both, c, weights, seed=None, gds=None, c_buf=None, wide=False, spread=False, tile=TILE):
    d = both.shape[1]
    chunk = 768 if spread else TILE
    toks = both.shape[0] // 2 if which == "own" else both.shape[0] // 8
    total = 4 * toks
    f = weights[0].shape[2]
    last = layer == 0
    struct = jax.ShapeDtypeStruct
    block = toks // tile
    lo, hi = {"own": (0, block), "oth": (block, 4 * block), "all": (0, 4 * block)}[which]

    def gathered(i, meta):
        t = i + lo
        b = t // block
        b = jnp.where(b == 0, meta[0], jnp.where(b <= meta[0], b - 1, b))
        return (b * block + t % block, 0)

    def paired(under):
        if which == "own":
            return lambda i, meta: (i + under * block, 0)

        def index(i, meta):
            row = gathered(i, meta)[0]
            return (row + (row // block + under) * block, 0)

        return index

    local = lambda i, meta: (i, 0)
    pair_in = [pl.BlockSpec((tile, d), paired(under)) for under in (0, 1)]
    rows_in = pl.BlockSpec((tile, d), local if which == "own" else gathered)
    rows_out = pl.BlockSpec((tile, d), local if which == "own" and not wide else gathered)
    any_spec = pl.BlockSpec(memory_space=pl.ANY)
    part = f // 4 if spread else f
    grads = [(d, part), (part, d), (d, d), (d, d)]
    args = [meta, both, both, c, *weights]
    in_specs = pair_in + [rows_in] + [any_spec] * 4
    aliases = {}
    if seed is not None:
        args += list(seed)
        in_specs += [any_spec] * 4
    n_c = 0 if last else 1
    for buf, pos in ((c_buf, 0), (gds, n_c)):
        if buf is not None:
            aliases[len(args)] = pos
            args.append(buf)
            in_specs.append(any_spec)
    extra = len(args) - 8
    c_shape = (toks if which == "own" and not wide else total, d)
    res = pl.pallas_call(
        functools.partial(bwd_kernel, chunk, last, 0 if seed is None else 1, spread, extra),
        grid_spec=pltpu.PrefetchScalarGridSpec(
            num_scalar_prefetch=1,
            grid=(hi - lo,),
            in_specs=in_specs,
            out_specs=[rows_out] * n_c + [pl.BlockSpec((tile, d), lambda i, meta: (i + lo, 0))] + [any_spec] * 4,
            scratch_shapes=[pltpu.VMEM(w.shape[1:], BF16) for w in weights]
            + [pltpu.VMEM(g, F32) for g in grads]
            + [pltpu.SemaphoreType.DMA((4 + 2 * (f // chunk),))] * 3
            + ([pltpu.VMEM((tile, f), BF16)] * 2 if spread else []),
        ),
        out_shape=[struct(c_shape, F32)] * n_c + [struct((total, d), F32)] + [struct(g, F32) for g in grads],
        input_output_aliases=aliases,
        compiler_params=pltpu.CompilerParams(vmem_limit_bytes=VMEM_MAX),
        cost_estimate=memory_cost(30 * (hi - lo)),
        name="layer_bwd",
    )(*args)
    return (None if last else res[0]), res[n_c], tuple(res[-4:])


def table_kernel(first, layers, seg, unroll, order_ref, list_ref, *refs):
    sources = [refs[2 * l:2 * l + 2] for l in range(layers)]
    out_ref, acc, buf, in_sem, out_sem = refs[-5:]
    homes, cap = list_ref.shape[0], list_ref.shape[1] // 2
    half = homes // 2
    toks = sources[0][0].shape[0] // half

    def low(h):
        start = list_ref[order_ref[h], cap + 1]
        return jnp.minimum(start - start % 8, toks - seg)

    def load(l, h):
        at = pl.multiple_of((h % half) * toks + low(h), 8)
        return pltpu.make_async_copy(sources[l][h // half].at[pl.ds(at, seg), :], buf.at[l % 2, h], in_sem.at[l % 2, h])

    def store(l):
        return pltpu.make_async_copy(acc.at[l % 2], out_ref.at[first - l], out_sem.at[l % 2])

    for h in range(homes):
        load(0, h).start()
    for l in range(layers):
        if l + 1 < layers:
            for h in range(homes):
                load(l + 1, h).start()
        if l >= 2:
            store(l - 2).wait()
        acc[l % 2] = jnp.zeros_like(acc[l % 2])
        for h in range(homes):
            load(l, h).wait()
            home = order_ref[h]
            count = list_ref[home, cap]
            off = list_ref[home, cap + 1] - low(h)

            def add(j, h=h, l=l, off=off, home=home):
                at = pl.ds(list_ref[home, j], 1)
                acc[l % 2, at, :] += buf[l % 2, h, pl.ds(off + j, 1), :]

            def many(t, _, add=add):
                for v in range(unroll):
                    add(t * unroll + v)
                return 0

            def one(j, _, add=add):
                add(j)
                return 0

            full = count // unroll
            lax.fori_loop(0, full, many, 0)
            lax.fori_loop(full * unroll, count, one, 0)
        store(l).start()
    for l in range(max(layers - 2, 0), layers):
        store(l).wait()


def table_grad(first, layers_all, rows, order, lists, sources, prev):
    d = sources[0][0].shape[1]
    homes, cap = lists.shape[0], lists.shape[1] // 2
    seg = cap + 8
    any_spec = pl.BlockSpec(memory_space=pl.ANY)
    args = [arr for src in sources for arr in src]
    aliases = {}
    if prev is not None:
        aliases = {2 + len(args): 0}
        args.append(prev)
    return pl.pallas_call(
        functools.partial(table_kernel, first, len(sources), seg, 8),
        grid_spec=pltpu.PrefetchScalarGridSpec(
            num_scalar_prefetch=2,
            in_specs=[any_spec] * len(args),
            out_specs=any_spec,
            scratch_shapes=[
                pltpu.VMEM((2, rows, d), F32),
                pltpu.VMEM((2, homes, seg, d), F32),
                pltpu.SemaphoreType.DMA((2, homes)),
                pltpu.SemaphoreType.DMA((2,)),
            ],
        ),
        out_shape=jax.ShapeDtypeStruct((layers_all, rows, d), F32),
        input_output_aliases=aliases,
        compiler_params=pltpu.CompilerParams(vmem_limit_bytes=VMEM_MAX),
        cost_estimate=memory_cost(2 * len(sources)),
        name="table_grad",
    )(order, lists, *args)


def pick_rows(pos_ref, pick, step=256):
    n = pick.shape[1]
    rows = lax.broadcasted_iota(jnp.int32, (step, n), 0)
    for k in range(n // step):
        pick[pl.ds(k * step, step), :] = jnp.where(pos_ref[...] == rows + k * step, 1.0, 0.0).astype(BF16)


def sort_kernel(pos_ref, x_ref, y_ref, xs_ref, ys_ref, pick):
    pick_rows(pos_ref, pick)
    xs_ref[...] = nn(pick[...], x_ref[...]).astype(BF16)
    ys_ref[...] = nn(pick[...], y_ref[...]).astype(BF16)


def sort_rows(pos, x, y):
    n, d = x.shape
    return pl.pallas_call(
        sort_kernel,
        out_shape=[jax.ShapeDtypeStruct((n, d), BF16)] * 2,
        scratch_shapes=[pltpu.VMEM((n, n), BF16)],
        compiler_params=pltpu.CompilerParams(vmem_limit_bytes=24 << 20),
        cost_estimate=memory_cost(1),
        name="sort_rows",
    )(pos[None, :], x, y)


def sum_kernel(count, *refs):
    outs = refs[-count:]
    for k in range(count):
        outs[k][...] = refs[k][...] + refs[count + k][...]


def sum_grads(layer, layers, mine, other, prev, steps=8):
    count = len(mine)
    ins, outs = [], []
    for arr in mine:
        block = (arr.shape[0] // steps, arr.shape[1])
        ins.append(pl.BlockSpec(block, lambda i: (i, 0)))
        outs.append(pl.BlockSpec((None,) + block, lambda i: (layer, i, 0)))
    args = list(mine) + list(other)
    aliases = {}
    if prev is not None:
        aliases = {len(args) + k: k for k in range(count)}
        args += list(prev)
    return pl.pallas_call(
        functools.partial(sum_kernel, count),
        grid=(steps,),
        in_specs=ins + ins + [pl.BlockSpec(memory_space=pl.ANY)] * len(aliases),
        out_specs=outs,
        out_shape=[jax.ShapeDtypeStruct((layers,) + arr.shape, F32) for arr in mine],
        input_output_aliases=aliases,
        compiler_params=pltpu.CompilerParams(vmem_limit_bytes=VMEM_MAX),
        cost_estimate=memory_cost(2),
        name="sum_grads",
    )(*args)


def piece_kernel(core_ref, *refs):
    mine, other, outs = refs[:4], refs[4:8], refs[-3:]
    for k in range(2):
        outs[0][k] = mine[k][...] + other[k][...]
        outs[1 + k][...] = mine[2 + k][...] + other[2 + k][...]


def sum_pieces(layer, core, mine, other, prev, steps=4):
    d = mine[0].shape[1]
    rows = d // 2 // steps
    half = pl.BlockSpec((rows, d), lambda i, core: (i + core[0] * steps, 0))
    full = pl.BlockSpec((2 * rows, d), lambda i, core: (i, 0))
    stack = pl.BlockSpec((None, 2 * rows, d), lambda i, core: (layer, i, 0))
    any_spec = pl.BlockSpec(memory_space=pl.ANY)
    return pl.pallas_call(
        piece_kernel,
        grid_spec=pltpu.PrefetchScalarGridSpec(
            num_scalar_prefetch=1,
            grid=(steps,),
            in_specs=[half, half, full, full] * 2 + [any_spec] * 2,
            out_specs=[pl.BlockSpec((2, rows, d), lambda i, core: (0, i, 0)), stack, stack],
        ),
        out_shape=[jax.ShapeDtypeStruct((2, d // 2, d), F32)] + [jax.ShapeDtypeStruct(p.shape, F32) for p in prev],
        input_output_aliases={9: 1, 10: 2},
        compiler_params=pltpu.CompilerParams(vmem_limit_bytes=VMEM_MAX),
        cost_estimate=memory_cost(1),
        name="sum_pieces",
    )(core, *mine, *other, *prev)


def place_kernel(in_ref, *refs):
    up, down = refs[-2:]
    per, _, rows, d = in_ref.shape
    for j in range(per):
        up[pl.ds((j % CORES) * rows, rows), pl.ds((j // CORES) * d, d)] = in_ref[j, 0]
        down[pl.ds(j * rows, rows), :] = in_ref[j, 1]


def place_pieces(layer, pieces, prev, steps=4):
    n, _, rows, d = pieces.shape
    per = n // steps
    any_spec = pl.BlockSpec(memory_space=pl.ANY)
    return pl.pallas_call(
        place_kernel,
        grid=(steps,),
        in_specs=[pl.BlockSpec((per, 2, rows, d), lambda i: (i, 0, 0, 0))] + [any_spec] * 2,
        out_specs=[
            pl.BlockSpec((None, CORES * rows, per // CORES * d), lambda i: (layer, 0, i)),
            pl.BlockSpec((None, per * rows, d), lambda i: (layer, i, 0)),
        ],
        out_shape=[jax.ShapeDtypeStruct(p.shape, F32) for p in prev],
        input_output_aliases={1: 0, 2: 1},
        compiler_params=pltpu.CompilerParams(vmem_limit_bytes=VMEM_MAX),
        cost_estimate=memory_cost(1),
        name="place_pieces",
    )(pieces, *prev)


def after(value, *deps):
    return lax.optimization_barrier((value,) + deps)[0]


def solution(mesh):
    shards = mesh.shape["emb"]
    chips = shards // CORES
    same_core = [[chip * CORES + core for chip in range(chips)] for core in range(CORES)]
    swap = [(d, d ^ 1) for d in range(shards)]

    def device_step(tok_ids, x_in, d_out, ple_tables, w_up, w_down, w_gate, w_proj):
        layers, rows_dev, width = ple_tables.shape
        toks = tok_ids.shape[0]
        cap = toks // CAP_DIV
        me = lax.axis_index("emb")
        core, chip = me % CORES, me // CORES
        weights = (w_up, w_down, w_gate, w_proj)
        i32 = jnp.int32

        def gather_core(arr):
            return lax.all_gather(arr, "emb", axis_index_groups=same_core, tiled=True)

        owner = tok_ids // rows_dev
        local_row = tok_ids - owner * rows_dev
        hot = jax.nn.one_hot(owner, shards, dtype=i32)
        run = jnp.cumsum(hot, axis=0)
        rank = jnp.sum((run - hot) * hot, axis=1)
        counts = run[-1]
        starts = jnp.cumsum(counts) - counts
        pos = jnp.sum(starts[None, :] * hot, axis=1) + rank
        x_own, dy_own = sort_rows(pos, x_in, d_out)
        dy_all = gather_core(dy_own)
        owner = after(owner, dy_own)
        req = jnp.zeros((shards * 2 * cap,), i32).at[owner * (2 * cap) + rank].set(local_row).reshape(shards, 2 * cap)
        req = req.at[:, cap].set(counts).at[:, cap + 1].set(starts)
        req = lax.all_to_all(req, "emb", 0, 0, tiled=True)
        seat = jnp.arange(toks, dtype=i32)[:, None]
        lies = jnp.logical_and(seat >= starts[None, :], seat < (starts + counts)[None, :]).astype(i32)
        rel = jnp.arange(shards, dtype=i32) ^ me
        take = jnp.sum(lies * (rel * cap - starts)[None, :], axis=1, keepdims=True) + seat
        meta = [jnp.stack([chip, l]).astype(i32) for l in range(layers)]
        core_arr = core.astype(i32)[None]
        order = jnp.arange(chips, dtype=i32)
        order = jnp.where(order == 0, chip, jnp.where(order <= chip, order - 1, order)) * CORES
        order = jnp.concatenate([order + core, order + 1 - core])
        req, take, x_own, meta, core_arr, order, rel = lax.optimization_barrier((req, take, x_own, meta, core_arr, order, rel))

        first = serve_rows(ple_tables, 0, 1, rel, req)[0].reshape(shards, cap, width)
        got = [first[0]]
        for s in range(1, shards):
            got.append(lax.ppermute(first[s], "emb", [(d, d ^ s) for d in range(shards)]))
        served = serve_rows(ple_tables, 1, layers - 1, after(rel, first), req)
        both = start_layers(take, x_own, served, got, weights, shards)

        x_out = top_forward(pos, both[-1], weights)
        split = layers - SPLIT
        c_own, seeds, gds_buf, c_buf = after(dy_own, x_out), {}, {}, None
        for l in reversed(range(split, layers)):
            c_own, gds_buf[l], seeds[l] = layer_bwd(l, meta[l], "own", both[l], c_own, weights, wide=l == split, spread=l in SPREAD)
            if l == split:
                c_buf = c_own
        c = after(dy_all, gds_buf[split])
        both_all = [gather_core(both[l]) for l in range(layers)]
        gds, part, other = {}, {}, {}
        swapped, sums, pieces = {}, None, {}
        for l in reversed(range(layers)):
            if l >= split:
                c_new, gds[l], part[l] = layer_bwd(l, meta[l], "oth", both_all[l], c, weights, seed=seeds[l], gds=gds_buf[l], c_buf=c_buf if l == split else None, spread=l in SPREAD)
            else:
                c_new, gds[l], part[l] = layer_bwd(l, meta[l], "all", both_all[l], c, weights, spread=l in SPREAD)
            moved = []
            for arr in (gds[l], *part[l]):
                moved.append(lax.ppermute(arr, "emb", swap))
            other[l], swapped[l] = moved[0], tuple(moved[1:])
            if l + 1 < layers:
                _, other[l + 1], theirs = lax.optimization_barrier((gds[l], other[l + 1], swapped[l + 1]))
                if l + 1 in SPREAD:
                    piece, *gates = sum_pieces(l + 1, core_arr, part[l + 1], theirs, sums[2:])
                    sums = list(sums[:2]) + gates
                    pieces[l + 1] = lax.all_gather(piece, "emb")
                else:
                    sums = sum_grads(l + 1, layers, part[l + 1], theirs, sums)
                if l > 0:
                    c_new, other[l + 1], sums = lax.optimization_barrier((c_new, other[l + 1], sums))
            c = c_new

        def placed(l, sums, dep):
            return list(place_pieces(l, after(pieces[l], dep), sums[:2])) + list(sums[2:])

        sums = placed(SPREAD[0], sums, sums[-1])
        tables = table_grad(layers - 1, layers, rows_dev, order, req, [(after(gds[l], sums[0]), other[l]) for l in reversed(range(layers))], None)
        for l in SPREAD[1:-1]:
            sums = placed(l, sums, tables)
        sums = sum_grads(0, layers, part[0], after(swapped[0], sums[0], tables), sums)
        sums = placed(SPREAD[-1], sums, sums[-1])
        return (x_out, tables, *sums)

    return jax.shard_map(
        device_step,
        mesh=mesh,
        in_specs=(P("emb"), P("emb", None), P("emb", None), P(None, "emb", None), P(), P(), P(), P()),
        out_specs=(P("emb", None), P(None, "emb", None), P(), P(), P(), P()),
        check_vma=False,
    )
```

```python
import functools

import jax
import jax.numpy as jnp
from jax import lax
from jax.experimental import pallas as pl
from jax.experimental.pallas import tpu as pltpu
from jax.sharding import PartitionSpec as P


EPS = 1e-6
CAP_DIV = 4
CORES = 2
F32 = jnp.float32
BF16 = jnp.bfloat16
GELU_A = 0.7978845608028654
GELU_B = 0.044715 * GELU_A
VMEM_MAX = 67043328
TILE = 512
MEMORY_UNIT = 500000000
SPLIT = 3
EARLY = 1
SPREAD = (3, 2, 1)


def nn(a, b):
    return jnp.dot(a, b, preferred_element_type=F32)


def nt(a, b):
    return lax.dot_general(a, b, (((1,), (1,)), ((), ())), preferred_element_type=F32)


def tn(a, b):
    return lax.dot_general(a, b, (((0,), (0,)), ((), ())), preferred_element_type=F32)


def gelu_parts(h):
    sq = h * h
    return 0.5 * jnp.tanh(h * (GELU_B * sq + GELU_A)) + 0.5, sq


def gelu(h):
    return h * gelu_parts(h)[0]


def gelu_slope(h, half, sq):
    return half + (h * (half - half * half)) * ((6 * GELU_B) * sq + 2 * GELU_A)


def norm_rows(x_ref):
    xw = x_ref[...].astype(F32)
    r = lax.rsqrt(jnp.mean(xw * xw, axis=-1, keepdims=True) + EPS)
    return xw, r, (xw * r).astype(BF16)


def memory_cost(units):
    return pl.CostEstimate(flops=units * MEMORY_UNIT, bytes_accessed=units * MEMORY_UNIT, transcendentals=0)


def forward_rows(chunk, x_ref, e, w_ref):
    up_ref, down_ref, gate_ref, proj_ref = w_ref
    xw, _, u = norm_rows(x_ref)
    z = nn(u, gate_ref[...]).astype(BF16).astype(F32)
    s = (gelu(z).astype(BF16).astype(F32) * e.astype(F32)).astype(BF16)
    m = None
    for k in range(up_ref.shape[1] // chunk):
        cols = pl.ds(k * chunk, chunk)
        a = gelu(nn(u, up_ref[:, cols]).astype(BF16).astype(F32)).astype(BF16)
        part = nn(a, down_ref[cols, :])
        m = part if m is None else m + part
    q = nn(s, proj_ref[...]).astype(BF16)
    return (xw + m.astype(BF16).astype(F32) + q.astype(F32)).astype(BF16)


def start_kernel(chunk, tile, shards, take_ref, x_ref, served_ref, *refs):
    got, refs = refs[:EARLY * shards], refs[EARLY * shards:]
    w_ref, refs = refs[:4], refs[4:]
    layer = pl.program_id(0)
    layers = served_ref.shape[0] + EARLY
    both_out = refs[:layers]
    recv, pick, x_cur, e_buf, x_buf, send_sem, recv_sem, own_sem, e_sem, x_sem, first_sem = refs[layers:]
    slots = served_ref.shape[1]
    toks = x_ref.shape[0]
    cap = slots // shards
    me = lax.axis_index("emb")

    def copy_in(l, s):
        rows = pl.ds(s * cap, cap)
        dst = recv.at[l, rows, :]
        if l < EARLY:
            return pltpu.make_async_copy(got[l * shards + s], dst, first_sem.at[l * shards + s])
        src = served_ref.at[l - EARLY, rows, :]
        if s == 0:
            return pltpu.make_async_copy(src, dst, own_sem.at[l])
        peer, bit = 0, 1
        while bit < shards:
            peer = peer + bit * ((me // bit + s // bit) % 2)
            bit *= 2
        return pltpu.make_async_remote_copy(
            src_ref=src,
            dst_ref=dst,
            send_sem=send_sem.at[l, s - 1],
            recv_sem=recv_sem.at[l, s - 1],
            device_id=(peer,),
            device_id_type=pl.DeviceIdType.MESH,
        )

    def save_e(l):
        return pltpu.make_async_copy(e_buf.at[l % 2], both_out[l].at[pl.ds(toks, toks), :], e_sem.at[l])

    def save_x(l):
        src = x_ref if l < 0 else x_buf.at[l % 2]
        return pltpu.make_async_copy(src, both_out[l + 1].at[pl.ds(0, toks), :], x_sem.at[l + 1])

    @pl.when(layer == 0)
    def _():
        for l in range(layers):
            for s in range(shards):
                copy_in(l, s).start()
        save_x(-1).start()
        x_cur[...] = x_ref[...]
        lanes = lax.broadcasted_iota(jnp.int32, (toks, cap), 1)
        for k in range(shards):
            pick[:, pl.ds(k * cap, cap)] = jnp.where(take_ref[...] == lanes + k * cap, 1.0, 0.0).astype(BF16)

    for l in range(layers):

        @pl.when(layer == l)
        def _(l=l):
            copy_in(l, 0).wait()
            for s in range(1, shards):
                copy_in(l, s).wait_recv() if l >= EARLY else copy_in(l, s).wait()
            if l >= 2:
                save_e(l - 2).wait()
                save_x(l - 2).wait()

    half = layer % 2
    e_buf[half] = nn(pick[...], recv[layer]).astype(BF16)

    @pl.when(layer < layers - 1)
    def _():
        for t in range(toks // tile):
            rows = pl.ds(t * tile, tile)
            x_new = forward_rows(chunk, x_cur.at[rows, :], e_buf[half, rows, :], w_ref)
            x_buf[half, rows, :] = x_new
            x_cur[rows, :] = x_new

    for l in range(layers):

        @pl.when(layer == l)
        def _(l=l):
            save_e(l).start()
            if l < layers - 1:
                save_x(l).start()

    @pl.when(layer == layers - 1)
    def _():
        for l in range(EARLY, layers):
            for s in range(1, shards):
                copy_in(l, s).wait_send()
        save_x(-1).wait()
        save_e(layers - 2).wait()
        save_x(layers - 2).wait()
        save_e(layers - 1).wait()


def start_layers(take, x, served, got, weights, shards, tile=TILE, chunk=1024):
    n, d = x.shape
    layers, slots = served.shape[0] + EARLY, served.shape[1]
    any_spec = pl.BlockSpec(memory_space=pl.ANY)
    whole = lambda arr: pl.BlockSpec(arr.shape, lambda i: (0, 0), pipeline_mode=pl.Buffered(1))
    wspec = lambda w: pl.BlockSpec((None,) + w.shape[1:], lambda i: (i, 0, 0))
    return pl.pallas_call(
        functools.partial(start_kernel, chunk, tile, shards),
        grid=(layers,),
        in_specs=[whole(take), whole(x)] + [any_spec] * (1 + len(got)) + [wspec(w) for w in weights],
        out_specs=[any_spec] * layers,
        out_shape=[jax.ShapeDtypeStruct((2 * n, d), BF16)] * layers,
        scratch_shapes=[
            pltpu.VMEM((layers, slots, d), BF16),
            pltpu.VMEM((n, slots), BF16),
            pltpu.VMEM((n, d), BF16),
            pltpu.VMEM((2, n, d), BF16),
            pltpu.VMEM((2, n, d), BF16),
            pltpu.SemaphoreType.DMA((layers, shards - 1)),
            pltpu.SemaphoreType.DMA((layers, shards - 1)),
            pltpu.SemaphoreType.DMA((layers,)),
            pltpu.SemaphoreType.DMA((layers,)),
            pltpu.SemaphoreType.DMA((layers,)),
            pltpu.SemaphoreType.DMA((EARLY * shards,)),
        ],
        compiler_params=pltpu.CompilerParams(vmem_limit_bytes=VMEM_MAX, has_side_effects=True),
        cost_estimate=memory_cost(100),
        name="start_layers",
    )(take, x, served, *got, *weights)


def top_kernel(chunk, tile, pos_ref, x_ref, e_ref, *refs):
    w_ref, (out_ref, last, pick) = refs[:4], refs[4:]
    n = pos_ref.shape[1]
    for t in range(n // tile):
        rows = pl.ds(t * tile, tile)
        last[rows, :] = forward_rows(chunk, x_ref.at[rows, :], e_ref[rows, :], w_ref)
    pick_rows(pos_ref, pick)
    out_ref[...] = tn(pick[...], last[...]).astype(BF16)


def top_forward(pos, both, weights, tile=TILE, chunk=1024):
    n, d = both.shape[0] // 2, both.shape[1]
    half = lambda under: pl.BlockSpec((n, d), lambda i: (under, 0))
    wspec = lambda w: pl.BlockSpec((None,) + w.shape[1:], lambda i: (w.shape[0] - 1, 0, 0))
    row = pl.BlockSpec((1, n), lambda i: (0, 0))
    return pl.pallas_call(
        functools.partial(top_kernel, chunk, tile),
        grid=(1,),
        in_specs=[row, half(0), half(1)] + [wspec(w) for w in weights],
        out_specs=half(0),
        out_shape=jax.ShapeDtypeStruct((n, d), BF16),
        scratch_shapes=[pltpu.VMEM((n, d), BF16), pltpu.VMEM((n, n), BF16)],
        compiler_params=pltpu.CompilerParams(vmem_limit_bytes=VMEM_MAX),
        cost_estimate=memory_cost(30),
        name="top_forward",
    )(pos[None, :], both, both, *weights)


def gather_kernel(unroll, order_ref, idx_ref, table_ref, out_ref, rows, tmp):
    homes, cap = idx_ref.shape[0], idx_ref.shape[1] // 2

    @pl.when(pl.program_id(0) == 0)
    def _():
        rows[...] = jnp.zeros_like(rows)

    for h in range(homes):
        home = order_ref[h]

        def body(t, _, h=h, home=home):
            for v in range(unroll):
                j = t * unroll + v
                r = idx_ref[home, j]
                tmp[v] = table_ref[pl.ds(pl.multiple_of(r - (r & 7), 8), 8), :].astype(F32)
                rows[pl.ds(h * cap + j, 1), :] = tmp[v, pl.ds(r & 7, 1), :]
            return 0

        lax.fori_loop(0, (idx_ref[home, cap] + unroll - 1) // unroll, body, 0)
    out_ref[...] = rows[...].astype(BF16)


def serve_rows(tables, first, count, order, lists, unroll=16):
    _, rows, d = tables.shape
    homes, cap = lists.shape[0], lists.shape[1] // 2
    return pl.pallas_call(
        functools.partial(gather_kernel, unroll),
        grid_spec=pltpu.PrefetchScalarGridSpec(
            num_scalar_prefetch=2,
            grid=(count,),
            in_specs=[pl.BlockSpec((None, rows, d), lambda i, *_: (first + i, 0, 0))],
            out_specs=pl.BlockSpec((None, homes * cap, d), lambda i, *_: (i, 0, 0)),
            scratch_shapes=[pltpu.VMEM((homes * cap, d), F32), pltpu.VMEM((unroll, 8, d), F32)],
        ),
        out_shape=jax.ShapeDtypeStruct((count, homes * cap, d), BF16),
        compiler_params=pltpu.CompilerParams(vmem_limit_bytes=48 << 20),
        cost_estimate=memory_cost(2 * count),
        name="serve_rows",
    )(order, lists, tables)


def bwd_kernel(chunk, last, seeded, spread, extra, meta_ref, *refs):
    x_ref, e_ref, c_ref = refs[:3]
    w_hbm, seed_hbm = refs[3:7], refs[7:7 + 4 * seeded]
    refs = list(refs[7 + extra:])
    cn_ref = None if last else refs.pop(0)
    gds_ref, *refs = refs
    grad_hbm, w_ref, g_ref, (w_sem, s_sem, g_sem, *keep) = refs[:4], refs[4:8], refs[8:12], refs[12:]
    up_ref, down_ref, gate_ref, proj_ref = w_ref
    steps = up_ref.shape[1] // chunk
    step, n_steps = pl.program_id(0), pl.num_programs(0)
    cols = lambda k: pl.ds(k * chunk, chunk)

    def flush(a, k):
        part = lambda ref: ref if k is None else (ref.at[:, cols(k)] if a == 0 else ref.at[cols(k), :])
        return pltpu.make_async_copy(part(g_ref[a]), part(grad_hbm[a]), g_sem.at[a if k is None else 4 + 2 * k + a])

    @pl.when(step == 0)
    def _():
        loads = [pltpu.make_async_copy(w_hbm[a].at[meta_ref[1]], w_ref[a], w_sem.at[a]) for a in range(4)]
        loads += [pltpu.make_async_copy(seed_hbm[a], g_ref[a], s_sem.at[a]) for a in range(4 * seeded)]
        for load in loads:
            load.start()
        if not seeded:
            for ref in g_ref:
                ref[...] = jnp.zeros_like(ref)
        for load in loads:
            load.wait()

    started = []

    def accumulate(a, value, k=None):
        if k is None:
            g_ref[a][...] += value
        elif a == 0:
            g_ref[a][:, cols(k)] += value
        else:
            g_ref[a][cols(k), :] += value
        pl.when(step == n_steps - 1)(lambda: flush(a, k).start())
        started.append((a, k))

    xw, r, u = norm_rows(x_ref)
    c = c_ref[...].astype(F32)
    o = c.astype(BF16)

    def first(k):
        return nt(o, down_ref[cols(k), :]).astype(BF16), nn(u, up_ref[:, cols(k)]).astype(BF16)

    def middle(da, h):
        h = h.astype(F32)
        half, sq = gelu_parts(h)
        return (gelu_slope(h, half, sq) * da.astype(F32)).astype(BF16), (h * half).astype(BF16)

    def final(k, dh, a):
        if spread:
            keep[0][:, cols(k)] = dh
            keep[1][:, cols(k)] = a
        else:
            accumulate(0, tn(u, dh), k)
            accumulate(1, tn(a, o), k)
        return None if last else nt(dh, up_ref[:, cols(k)])

    pre = first(0)
    z = nn(u, gate_ref[...]).astype(BF16).astype(F32)
    ds = nt(o, proj_ref[...]).astype(BF16).astype(F32)
    e = e_ref[...].astype(F32)
    half, sq = gelu_parts(z)
    g = (z * half).astype(BF16).astype(F32)
    gds_ref[...] = g * ds
    s = (g * e).astype(BF16)
    dz = (gelu_slope(z, half, sq) * (e * ds).astype(BF16).astype(F32)).astype(BF16)
    accumulate(2, tn(u, dz))
    accumulate(3, tn(s, o))
    du = None if last else nt(dz, gate_ref[...])
    mid = None
    for k in range(steps):
        nxt = first(k + 1) if k + 1 < steps else None
        if mid is not None:
            part = final(k - 1, *mid)
            du = None if last else du + part
        mid = middle(*pre)
        pre = nxt
    part = final(steps - 1, *mid)
    if spread:
        width = g_ref[1].shape[0]
        mine = pl.ds(pl.multiple_of(meta_ref[0] * width, 128), width)
        accumulate(0, tn(u, keep[0][:, mine]))
        accumulate(1, tn(keep[1][:, mine], o))
    if not last:
        du = du + part
        cn_ref[...] = c + r * du - (r * r * r) * xw * jnp.mean(du * xw, axis=-1, keepdims=True)

    @pl.when(step == n_steps - 1)
    def _():
        for a, k in started:
            flush(a, k).wait()


def layer_bwd(layer, meta, which, both, c, weights, seed=None, gds=None, c_buf=None, wide=False, spread=False, tile=TILE):
    d = both.shape[1]
    chunk = 768 if spread else TILE
    toks = both.shape[0] // 2 if which == "own" else both.shape[0] // 8
    total = 4 * toks
    f = weights[0].shape[2]
    last = layer == 0
    struct = jax.ShapeDtypeStruct
    block = toks // tile
    lo, hi = {"own": (0, block), "oth": (block, 4 * block), "all": (0, 4 * block)}[which]

    def gathered(i, meta):
        t = i + lo
        b = t // block
        b = jnp.where(b == 0, meta[0], jnp.where(b <= meta[0], b - 1, b))
        return (ring_place(b) * block + t % block, 0)

    def paired(under):
        if which == "own":
            return lambda i, meta: (i + under * block, 0)

        def index(i, meta):
            row = gathered(i, meta)[0]
            return (row + (row // block + under) * block, 0)

        return index

    local = lambda i, meta: (i, 0)
    pair_in = [pl.BlockSpec((tile, d), paired(under)) for under in (0, 1)]
    rows_in = pl.BlockSpec((tile, d), local if which == "own" else gathered)
    rows_out = pl.BlockSpec((tile, d), local if which == "own" and not wide else gathered)
    any_spec = pl.BlockSpec(memory_space=pl.ANY)
    part = f // 4 if spread else f
    grads = [(d, part), (part, d), (d, d), (d, d)]
    args = [meta, both, both, c, *weights]
    in_specs = pair_in + [rows_in] + [any_spec] * 4
    aliases = {}
    if seed is not None:
        args += list(seed)
        in_specs += [any_spec] * 4
    n_c = 0 if last else 1
    for buf, pos in ((c_buf, 0), (gds, n_c)):
        if buf is not None:
            aliases[len(args)] = pos
            args.append(buf)
            in_specs.append(any_spec)
    extra = len(args) - 8
    c_shape = (toks if which == "own" and not wide else total, d)
    res = pl.pallas_call(
        functools.partial(bwd_kernel, chunk, last, 0 if seed is None else 1, spread, extra),
        grid_spec=pltpu.PrefetchScalarGridSpec(
            num_scalar_prefetch=1,
            grid=(hi - lo,),
            in_specs=in_specs,
            out_specs=[rows_out] * n_c + [pl.BlockSpec((tile, d), lambda i, meta: (i + lo, 0))] + [any_spec] * 4,
            scratch_shapes=[pltpu.VMEM(w.shape[1:], BF16) for w in weights]
            + [pltpu.VMEM(g, F32) for g in grads]
            + [pltpu.SemaphoreType.DMA((4 + 2 * (f // chunk),))] * 3
            + ([pltpu.VMEM((tile, f), BF16)] * 2 if spread else []),
        ),
        out_shape=[struct(c_shape, F32)] * n_c + [struct((total, d), F32)] + [struct(g, F32) for g in grads],
        input_output_aliases=aliases,
        compiler_params=pltpu.CompilerParams(vmem_limit_bytes=VMEM_MAX),
        cost_estimate=memory_cost(30 * (hi - lo)),
        name="layer_bwd",
    )(*args)
    return (None if last else res[0]), res[n_c], tuple(res[-4:])


def table_kernel(first, layers, seg, unroll, order_ref, list_ref, *refs):
    sources = [refs[2 * l:2 * l + 2] for l in range(layers)]
    out_ref, acc, buf, in_sem, out_sem = refs[-5:]
    homes, cap = list_ref.shape[0], list_ref.shape[1] // 2
    half = homes // 2
    toks = sources[0][0].shape[0] // half

    def low(h):
        start = list_ref[order_ref[h], cap + 1]
        return jnp.minimum(start - start % 8, toks - seg)

    def load(l, h):
        at = pl.multiple_of((h % half) * toks + low(h), 8)
        return pltpu.make_async_copy(sources[l][h // half].at[pl.ds(at, seg), :], buf.at[l % 2, h], in_sem.at[l % 2, h])

    def store(l):
        return pltpu.make_async_copy(acc.at[l % 2], out_ref.at[first - l], out_sem.at[l % 2])

    for h in range(homes):
        load(0, h).start()
    for l in range(layers):
        if l + 1 < layers:
            for h in range(homes):
                load(l + 1, h).start()
        if l >= 2:
            store(l - 2).wait()
        acc[l % 2] = jnp.zeros_like(acc[l % 2])
        for h in range(homes):
            load(l, h).wait()
            home = order_ref[h]
            count = list_ref[home, cap]
            off = list_ref[home, cap + 1] - low(h)

            def add(j, h=h, l=l, off=off, home=home):
                at = pl.ds(list_ref[home, j], 1)
                acc[l % 2, at, :] += buf[l % 2, h, pl.ds(off + j, 1), :]

            def many(t, _, add=add):
                for v in range(unroll):
                    add(t * unroll + v)
                return 0

            def one(j, _, add=add):
                add(j)
                return 0

            full = count // unroll
            lax.fori_loop(0, full, many, 0)
            lax.fori_loop(full * unroll, count, one, 0)
        store(l).start()
    for l in range(max(layers - 2, 0), layers):
        store(l).wait()


def table_grad(first, layers_all, rows, order, lists, sources, prev):
    d = sources[0][0].shape[1]
    homes, cap = lists.shape[0], lists.shape[1] // 2
    seg = cap + 8
    any_spec = pl.BlockSpec(memory_space=pl.ANY)
    args = [arr for src in sources for arr in src]
    aliases = {}
    if prev is not None:
        aliases = {2 + len(args): 0}
        args.append(prev)
    return pl.pallas_call(
        functools.partial(table_kernel, first, len(sources), seg, 8),
        grid_spec=pltpu.PrefetchScalarGridSpec(
            num_scalar_prefetch=2,
            in_specs=[any_spec] * len(args),
            out_specs=any_spec,
            scratch_shapes=[
                pltpu.VMEM((2, rows, d), F32),
                pltpu.VMEM((2, homes, seg, d), F32),
                pltpu.SemaphoreType.DMA((2, homes)),
                pltpu.SemaphoreType.DMA((2,)),
            ],
        ),
        out_shape=jax.ShapeDtypeStruct((layers_all, rows, d), F32),
        input_output_aliases=aliases,
        compiler_params=pltpu.CompilerParams(vmem_limit_bytes=VMEM_MAX),
        cost_estimate=memory_cost(2 * len(sources)),
        name="table_grad",
    )(order, lists, *args)


def pick_rows(pos_ref, pick, step=256):
    n = pick.shape[1]
    rows = lax.broadcasted_iota(jnp.int32, (step, n), 0)
    for k in range(n // step):
        pick[pl.ds(k * step, step), :] = jnp.where(pos_ref[...] == rows + k * step, 1.0, 0.0).astype(BF16)


def sort_kernel(pos_ref, x_ref, y_ref, xs_ref, ys_ref, pick):
    pick_rows(pos_ref, pick)
    xs_ref[...] = nn(pick[...], x_ref[...]).astype(BF16)
    ys_ref[...] = nn(pick[...], y_ref[...]).astype(BF16)


def sort_rows(pos, x, y):
    n, d = x.shape
    return pl.pallas_call(
        sort_kernel,
        out_shape=[jax.ShapeDtypeStruct((n, d), BF16)] * 2,
        scratch_shapes=[pltpu.VMEM((n, n), BF16)],
        compiler_params=pltpu.CompilerParams(vmem_limit_bytes=24 << 20),
        cost_estimate=memory_cost(1),
        name="sort_rows",
    )(pos[None, :], x, y)


def sum_kernel(count, *refs):
    outs = refs[-count:]
    for k in range(count):
        outs[k][...] = refs[k][...] + refs[count + k][...]


def sum_grads(layer, layers, mine, other, prev, steps=8):
    count = len(mine)
    ins, outs = [], []
    for arr in mine:
        block = (arr.shape[0] // steps, arr.shape[1])
        ins.append(pl.BlockSpec(block, lambda i: (i, 0)))
        outs.append(pl.BlockSpec((None,) + block, lambda i: (layer, i, 0)))
    args = list(mine) + list(other)
    aliases = {}
    if prev is not None:
        aliases = {len(args) + k: k for k in range(count)}
        args += list(prev)
    return pl.pallas_call(
        functools.partial(sum_kernel, count),
        grid=(steps,),
        in_specs=ins + ins + [pl.BlockSpec(memory_space=pl.ANY)] * len(aliases),
        out_specs=outs,
        out_shape=[jax.ShapeDtypeStruct((layers,) + arr.shape, F32) for arr in mine],
        input_output_aliases=aliases,
        compiler_params=pltpu.CompilerParams(vmem_limit_bytes=VMEM_MAX),
        cost_estimate=memory_cost(2),
        name="sum_grads",
    )(*args)


def piece_kernel(core_ref, *refs):
    mine, other, outs = refs[:4], refs[4:8], refs[-3:]
    for k in range(2):
        outs[0][k] = mine[k][...] + other[k][...]
        outs[1 + k][...] = mine[2 + k][...] + other[2 + k][...]


def sum_pieces(layer, core, mine, other, prev, steps=4):
    d = mine[0].shape[1]
    rows = d // 2 // steps
    half = pl.BlockSpec((rows, d), lambda i, core: (i + core[0] * steps, 0))
    full = pl.BlockSpec((2 * rows, d), lambda i, core: (i, 0))
    stack = pl.BlockSpec((None, 2 * rows, d), lambda i, core: (layer, i, 0))
    any_spec = pl.BlockSpec(memory_space=pl.ANY)
    return pl.pallas_call(
        piece_kernel,
        grid_spec=pltpu.PrefetchScalarGridSpec(
            num_scalar_prefetch=1,
            grid=(steps,),
            in_specs=[half, half, full, full] * 2 + [any_spec] * 2,
            out_specs=[pl.BlockSpec((2, rows, d), lambda i, core: (0, i, 0)), stack, stack],
        ),
        out_shape=[jax.ShapeDtypeStruct((2, d // 2, d), F32)] + [jax.ShapeDtypeStruct(p.shape, F32) for p in prev],
        input_output_aliases={9: 1, 10: 2},
        compiler_params=pltpu.CompilerParams(vmem_limit_bytes=VMEM_MAX),
        cost_estimate=memory_cost(1),
        name="sum_pieces",
    )(core, *mine, *other, *prev)


def place_kernel(in_ref, *refs):
    up, down = refs[-2:]
    per, _, rows, d = in_ref.shape
    for j in range(per):
        up[pl.ds((j % CORES) * rows, rows), pl.ds((j // CORES) * d, d)] = in_ref[j, 0]
        down[pl.ds(j * rows, rows), :] = in_ref[j, 1]


def place_pieces(layer, pieces, prev, steps=4):
    n, _, rows, d = pieces.shape
    per = n // steps
    any_spec = pl.BlockSpec(memory_space=pl.ANY)
    return pl.pallas_call(
        place_kernel,
        grid=(steps,),
        in_specs=[pl.BlockSpec((per, 2, rows, d), lambda i: (i, 0, 0, 0))] + [any_spec] * 2,
        out_specs=[
            pl.BlockSpec((None, CORES * rows, per // CORES * d), lambda i: (layer, 0, ring_place(i))),
            pl.BlockSpec((None, per * rows, d), lambda i: (layer, ring_place(i), 0)),
        ],
        out_shape=[jax.ShapeDtypeStruct(p.shape, F32) for p in prev],
        input_output_aliases={1: 0, 2: 1},
        compiler_params=pltpu.CompilerParams(vmem_limit_bytes=VMEM_MAX),
        cost_estimate=memory_cost(1),
        name="place_pieces",
    )(pieces, *prev)


def ring_place(chip):
    return chip ^ (chip // 2)


def after(value, *deps):
    return lax.optimization_barrier((value,) + deps)[0]


def solution(mesh):
    shards = mesh.shape["emb"]
    chips = shards // CORES
    ring = [ring_place(chip) for chip in range(chips)]
    same_core = [[chip * CORES + core for chip in ring] for core in range(CORES)]
    around = [[chip * CORES + core for chip in ring for core in range(CORES)]]
    swap = [(d, d ^ 1) for d in range(shards)]

    def device_step(tok_ids, x_in, d_out, ple_tables, w_up, w_down, w_gate, w_proj):
        layers, rows_dev, width = ple_tables.shape
        toks = tok_ids.shape[0]
        cap = toks // CAP_DIV
        me = lax.axis_index("emb")
        core, chip = me % CORES, me // CORES
        weights = (w_up, w_down, w_gate, w_proj)
        i32 = jnp.int32

        def gather_core(arr):
            return lax.all_gather(arr, "emb", axis_index_groups=same_core, tiled=True)

        owner = tok_ids // rows_dev
        local_row = tok_ids - owner * rows_dev
        hot = jax.nn.one_hot(owner, shards, dtype=i32)
        run = jnp.cumsum(hot, axis=0)
        rank = jnp.sum((run - hot) * hot, axis=1)
        counts = run[-1]
        starts = jnp.cumsum(counts) - counts
        pos = jnp.sum(starts[None, :] * hot, axis=1) + rank
        x_own, dy_own = sort_rows(pos, x_in, d_out)
        dy_all = gather_core(dy_own)
        owner = after(owner, dy_own)
        req = jnp.zeros((shards * 2 * cap,), i32).at[owner * (2 * cap) + rank].set(local_row).reshape(shards, 2 * cap)
        req = req.at[:, cap].set(counts).at[:, cap + 1].set(starts)
        req = lax.all_to_all(req, "emb", 0, 0, tiled=True)
        seat = jnp.arange(toks, dtype=i32)[:, None]
        lies = jnp.logical_and(seat >= starts[None, :], seat < (starts + counts)[None, :]).astype(i32)
        rel = jnp.arange(shards, dtype=i32) ^ me
        take = jnp.sum(lies * (rel * cap - starts)[None, :], axis=1, keepdims=True) + seat
        meta = [jnp.stack([chip, l]).astype(i32) for l in range(layers)]
        core_arr = core.astype(i32)[None]
        order = jnp.arange(chips, dtype=i32)
        order = jnp.where(order == 0, chip, jnp.where(order <= chip, order - 1, order)) * CORES
        order = jnp.concatenate([order + core, order + 1 - core])
        req, take, x_own, meta, core_arr, order, rel = lax.optimization_barrier((req, take, x_own, meta, core_arr, order, rel))

        first = serve_rows(ple_tables, 0, EARLY, rel, req)
        got = []
        for l in range(EARLY):
            blocks = first[l].reshape(shards, cap, width)
            got.append(blocks[0])
            for s in range(1, shards):
                got.append(lax.ppermute(blocks[s], "emb", [(d, d ^ s) for d in range(shards)]))
        served = serve_rows(ple_tables, EARLY, layers - EARLY, after(rel, first), req)
        both = start_layers(take, x_own, served, got, weights, shards)

        x_out = top_forward(pos, both[-1], weights)
        split = layers - SPLIT
        c_own, seeds, gds_buf, c_buf = after(dy_own, x_out), {}, {}, None
        for l in reversed(range(split, layers)):
            c_own, gds_buf[l], seeds[l] = layer_bwd(l, meta[l], "own", both[l], c_own, weights, wide=l == split, spread=l in SPREAD)
            if l == split:
                c_buf = c_own
        c = after(dy_all, gds_buf[split])
        both_all = [gather_core(both[l]) for l in range(layers)]
        gds, part, other = {}, {}, {}
        swapped, sums, pieces = {}, None, {}
        for l in reversed(range(layers)):
            if l >= split:
                c_new, gds[l], part[l] = layer_bwd(l, meta[l], "oth", both_all[l], c, weights, seed=seeds[l], gds=gds_buf[l], c_buf=c_buf if l == split else None, spread=l in SPREAD)
            else:
                c_new, gds[l], part[l] = layer_bwd(l, meta[l], "all", both_all[l], c, weights, spread=l in SPREAD)
            moved = []
            for arr in (gds[l], *part[l]):
                moved.append(lax.ppermute(arr, "emb", swap))
            other[l], swapped[l] = moved[0], tuple(moved[1:])
            if l + 1 < layers:
                _, other[l + 1], theirs = lax.optimization_barrier((gds[l], other[l + 1], swapped[l + 1]))
                if l + 1 in SPREAD:
                    piece, *gates = sum_pieces(l + 1, core_arr, part[l + 1], theirs, sums[2:])
                    sums = list(sums[:2]) + gates
                    pieces[l + 1] = lax.all_gather(piece, "emb", axis_index_groups=around)
                else:
                    sums = sum_grads(l + 1, layers, part[l + 1], theirs, sums)
                if l > 0:
                    c_new, other[l + 1], sums = lax.optimization_barrier((c_new, other[l + 1], sums))
            c = c_new

        def placed(l, sums, dep):
            return list(place_pieces(l, after(pieces[l], dep), sums[:2])) + list(sums[2:])

        sums = placed(SPREAD[0], sums, sums[-1])
        tables = table_grad(layers - 1, layers, rows_dev, order, req, [(after(gds[l], sums[0]), other[l]) for l in reversed(range(layers))], None)
        for l in SPREAD[1:-1]:
            sums = placed(l, sums, tables)
        sums = sum_grads(0, layers, part[0], after(swapped[0], sums[0], tables), sums)
        sums = placed(SPREAD[-1], sums, sums[-1])
        return (x_out, tables, *sums)

    return jax.shard_map(
        device_step,
        mesh=mesh,
        in_specs=(P("emb"), P("emb", None), P("emb", None), P(None, "emb", None), P(), P(), P(), P()),
        out_specs=(P("emb", None), P(None, "emb", None), P(), P(), P(), P()),
        check_vma=False,
    )
```
